32 devices in a mesh: dp: 4 (over y, x), vocab: 8 (over z, core).
Axes of the slice: x: 2, y: 2, z: 4, core: 2. Of those that a mesh axis runs over, the one named last changes fastest.
Arguments:
- hidden: bfloat16 [2048, 5120], P(('dp', 'vocab')), may hold values from -100 to 100
- tokens: int32 [2048], P('dp'), may hold values from 0 to 9215
- old_weight: bfloat16 [9216, 5120], P('vocab'), may hold values from -1 to 1
- new_weight: bfloat16 [9216, 5120], P('dp', 'vocab'), may hold values from -6 to 6
Outputs:
- logprob: float32 [2048], P(('dp', 'vocab'))
- engine_weight: bfloat16 [9216, 5120], P('vocab')
The draws below stay inside these ranges and needn't reach their ends.
All inputs are finite; a program needn't handle non-finite values.
Results may differ from the reference program's by a relative error of at most 0.001.
Values may be sent and summed in bfloat16 or wider, within the bound.
A program may use at most 128 MiB of HBM per device.

```python
import math
import jax
import jax.numpy as jnp
from jax import lax

D = 5120
VOCAB = 9216
GROUP_ROWS = 512
ROWS = 2048
N_DP = 4


def base_weight(key):
    first_key = jax.random.fold_in(jax.random.fold_in(key, 11), 0)
    weights = jax.random.normal(first_key, (VOCAB, D), jnp.float32) / math.sqrt(D)
    return jnp.clip(weights, -1.0, 1.0)


def draw_old_weight(key, part):
    return base_weight(key).astype(jnp.bfloat16)


def draw_hidden(key, part):
    keys = jax.random.split(jax.random.fold_in(key, 23), 1)
    values = 3.0 * jax.random.normal(keys[0], (ROWS, D), jnp.float32)
    return jnp.clip(values, -100.0, 100.0).astype(jnp.bfloat16)


def set_ends(array, own_key, smallest, high):
    spot = [jax.random.randint(jax.random.fold_in(own_key, axis), (), 0, length) for axis, length in enumerate(array.shape)]
    longest = array.shape.index(max(array.shape))
    neighbour = spot[:longest] + [(spot[longest] + 1) % array.shape[longest]] + spot[longest + 1:]
    return array.at[tuple(spot)].set(smallest).at[tuple(neighbour)].set(high)


def levels(stream_key, shape, shards, least, top_value):
    gain = 1.0
    for position, shards_of in shards:
        steps = jax.random.uniform(jax.random.fold_in(jax.random.fold_in(stream_key, 6), position), (shards_of,), jnp.float32, least / len(shards), top_value / len(shards))
        gain = gain * jnp.repeat(jnp.exp(steps), shape[position] // shards_of).reshape((-1,) + (1,) * (len(shape) - 1 - position))
    return gain


def bell_draw(key, shape, deviation, bound, shards=(), dtype=jnp.bfloat16):
    result = deviation * jax.random.normal(key, shape, jnp.float32)
    if shards:
        result = result * levels(key, shape, shards, -0.22, 0.18)
    return jnp.clip(result, -bound, bound).astype(dtype)


def setup_inputs(seed: int = 0) -> dict:
    key_of = jax.random.split(jax.random.key(seed), 5)
    hidden = draw_hidden(jax.random.fold_in(key_of[4], 71), 0)
    tokens = set_ends(jax.random.randint(key_of[1], (ROWS,), 0, VOCAB), jax.random.fold_in(key_of[1], 1), 0, VOCAB - 1).astype(jnp.int32)
    old_weight = draw_old_weight(jax.random.fold_in(key_of[4], 71), 0)
    new_weight = bell_draw(key_of[3], (VOCAB, D), 1.0, 6.0, ((0, 4), (1, 8)))
    return dict(hidden=hidden, tokens=tokens, old_weight=old_weight, new_weight=new_weight)


def reference(hidden, tokens, old_weight, new_weight):
    def one_group(operands):
        rows, ids = operands
        logits = jnp.dot(rows, old_weight.T, preferred_element_type=jnp.float32)
        top = jnp.max(logits, axis=1)
        total = jnp.sum(jnp.exp(logits - top[:, None]), axis=1)
        target = jnp.take_along_axis(logits, ids[:, None].astype(jnp.int32), axis=1)[:, 0]
        return target - top - jnp.log(total)

    grouped = hidden.reshape(N_DP, GROUP_ROWS, D)
    grouped_ids = tokens.reshape(N_DP, GROUP_ROWS)
    logprob = lax.map(one_group, (grouped, grouped_ids)).reshape(ROWS)
    return logprob, new_weight
```

```python
import jax
import jax.numpy as jnp
from jax import lax
from jax.sharding import PartitionSpec as P


def combined_all(part, axis, combine):
    gathered = jax.tree.map(lambda a: lax.all_gather(a, axis), part)

    def take(source):
        return jax.tree.map(lambda a: lax.dynamic_index_in_dim(a, source, 0, False), gathered)

    return lax.fori_loop(
        1, lax.axis_size(axis), lambda source, state: combine(state, take(source)), take(0)
    )


def join_stats(earlier, later):
    high = jnp.maximum(earlier[0], later[0])
    summed = earlier[1] * jnp.exp(earlier[0] - high) + later[1] * jnp.exp(later[0] - high)
    return (high, summed, earlier[2] + later[2])


def on_device(hidden, tokens, old_weight, new_weight):
    ranks = lax.axis_size("vocab")
    rank = lax.axis_index("vocab")
    vocab_rows = old_weight.shape[0]
    first_id = rank * vocab_rows
    own_rows = hidden.shape[0]
    logits = lax.dot_general(
        lax.all_gather(hidden, "vocab", axis=0, tiled=True),
        old_weight,
        (((1,), (1,)), ((), ())),
        preferred_element_type=jnp.float32,
    )
    highest = jnp.max(logits, axis=1)
    summed = jnp.sum(jnp.exp(logits - highest[:, None]), axis=1)
    wanted = tokens - first_id
    columns = lax.broadcasted_iota(jnp.int32, logits.shape, 1)
    target = jnp.sum(jnp.where(columns == wanted[:, None], logits, 0.0), axis=1)
    stats = jnp.stack([highest, summed, target], axis=0)
    highest, summed, target = (stats[0], stats[1], stats[2])
    highest, summed, target = combined_all((highest, summed, target), "vocab", join_stats)
    row_first = rank * own_rows
    highest = lax.dynamic_slice_in_dim(highest, row_first, own_rows)
    summed = lax.dynamic_slice_in_dim(summed, row_first, own_rows)
    target = lax.dynamic_slice_in_dim(target, row_first, own_rows)
    logprob = target - highest - jnp.log(summed)
    replicas = lax.axis_size("dp")
    trainer_rows, trainer_cols = new_weight.shape
    owners = ranks // replicas
    piece = trainer_rows // (owners * replicas)
    chunks = 2
    part = piece // chunks
    rows = new_weight.reshape(owners, replicas, chunks, part, trainer_cols)
    gathered = []
    for chunk in range(chunks):
        mine = jnp.swapaxes(rows[:, :, chunk], 0, 1)
        mine = lax.all_to_all(mine, "dp", split_axis=0, concat_axis=0, tiled=True)
        mine = mine.reshape(ranks, part, trainer_cols)
        mine = lax.all_to_all(mine, "vocab", split_axis=0, concat_axis=0, tiled=True)
        gathered.append(lax.all_gather(mine, "dp", axis=0))
    complete = jnp.stack(gathered, axis=1)
    engine_weight = jnp.swapaxes(complete, 2, 3).reshape(vocab_rows, ranks * trainer_cols)
    return (logprob, engine_weight)


def solution(mesh):
    return jax.shard_map(
        on_device,
        mesh=mesh,
        in_specs=(P(("dp", "vocab"), None), P("dp"), P("vocab", None), P("dp", "vocab")),
        out_specs=(P(("dp", "vocab")), P("vocab", None)),
        check_vma=False,
    )
```

```python
import jax
import jax.numpy as jnp
from jax import lax
from jax.experimental import pallas as pl
from jax.experimental.pallas import tpu as pltpu
from jax.sharding import PartitionSpec as P


def place_first(piece_ref, out_ref):
    cols = piece_ref.shape[3]
    for source in range(piece_ref.shape[1]):
        out_ref[:, source * cols : (source + 1) * cols] = piece_ref[0, source]


def place_next(piece_ref, whole_ref, out_ref):
    place_first(piece_ref, out_ref)


def place(piece, whole, chunk, chunks):
    blocks, ranks, part, cols = piece.shape
    out = jax.ShapeDtypeStruct((blocks * chunks * part, ranks * cols), piece.dtype)
    in_specs = [pl.BlockSpec((1, ranks, part, cols), lambda k: (k, 0, 0, 0))]
    operands = (piece,)
    if whole is not None:
        in_specs.append(pl.BlockSpec(memory_space=pl.ANY))
        operands = (piece, whole)
    return pl.pallas_call(
        place_first if whole is None else place_next,
        grid=(blocks,),
        out_shape=out,
        in_specs=in_specs,
        out_specs=pl.BlockSpec((part, ranks * cols), lambda k: (k * chunks + chunk, 0)),
        input_output_aliases={} if whole is None else {1: 0},
        compiler_params=pltpu.CompilerParams(vmem_limit_bytes=56 * 1024 * 1024),
        cost_estimate=pl.CostEstimate(
            flops=0, bytes_accessed=2 * piece.size * piece.dtype.itemsize, transcendentals=0
        ),
    )(*operands)


def on_device(hidden, tokens, old_weight, new_weight):
    ranks = lax.axis_size("vocab")
    replicas = lax.axis_size("dp")
    rank = lax.axis_index("vocab")
    vocab_rows = old_weight.shape[0]
    first_id = rank * vocab_rows
    own_rows = hidden.shape[0]

    trainer_rows, trainer_cols = new_weight.shape
    owners = ranks // replicas
    chunks = 2
    part = trainer_rows // (owners * replicas * chunks)
    rows = new_weight.reshape(owners, replicas, chunks, part, trainer_cols)
    gathered = []
    for chunk in range(chunks):
        mine = jnp.swapaxes(rows[:, :, chunk], 0, 1)
        mine = lax.all_to_all(mine, "dp", split_axis=0, concat_axis=0, tiled=True)
        mine = mine.reshape(ranks, part, trainer_cols)
        mine = lax.all_to_all(mine, "vocab", split_axis=0, concat_axis=0, tiled=True)
        if chunk == chunks - 1:
            mine, hidden = lax.optimization_barrier((mine, hidden))
        gathered.append(lax.all_gather(mine, "dp", axis=0))

    blocks = [hidden]
    for shift in range(2, ranks, 2):
        ring = [(i, (i + shift) % ranks) for i in range(ranks)]
        blocks.append(lax.ppermute(hidden, "vocab", ring))
    swap = [(i, i ^ 1) for i in range(ranks)]
    blocks += [lax.ppermute(block, "vocab", swap) for block in blocks]
    steps = 2 * jnp.arange(ranks // 2)
    order = jnp.concatenate([(rank - steps) % ranks, ((rank ^ 1) - steps) % ranks])
    place_of = jnp.argmax(order[None, :] == jnp.arange(ranks)[:, None], axis=1)

    logits = lax.dot_general(
        jnp.concatenate(blocks, axis=0),
        old_weight,
        (((1,), (1,)), ((), ())),
        preferred_element_type=jnp.float32,
    )
    highest = jnp.max(logits, axis=1)
    summed = jnp.sum(jnp.exp(logits - highest[:, None]), axis=1)
    wanted = tokens.reshape(ranks, own_rows)[order].reshape(-1) - first_id
    columns = lax.broadcasted_iota(jnp.int32, logits.shape, 1)
    target = jnp.sum(jnp.where(columns == wanted[:, None], logits, 0.0), axis=1)
    stats = jnp.stack([highest, summed, target], axis=0).reshape(3, ranks, own_rows)
    stats = jnp.swapaxes(stats, 0, 1)[place_of]
    aligned = trainer_cols % 128 == 0 and part % 16 == 0
    engine_weight = None
    if aligned:
        engine_weight = place(gathered[0], None, 0, chunks)
        engine_weight, stats = lax.optimization_barrier((engine_weight, stats))
    stats = lax.all_to_all(stats, "vocab", split_axis=0, concat_axis=0, tiled=True)
    top = jnp.max(stats[:, 0], axis=0)
    total = jnp.sum(stats[:, 1] * jnp.exp(stats[:, 0] - top), axis=0)
    logprob = jnp.sum(stats[:, 2], axis=0) - top - jnp.log(total)

    if aligned:
        for chunk in range(1, chunks):
            engine_weight = place(gathered[chunk], engine_weight, chunk, chunks)
    else:
        complete = jnp.stack(gathered, axis=1)
        engine_weight = jnp.swapaxes(complete, 2, 3).reshape(vocab_rows, ranks * trainer_cols)
    return (logprob, engine_weight)


def solution(mesh):
    return jax.shard_map(
        on_device,
        mesh=mesh,
        in_specs=(P(("dp", "vocab"), None), P("dp"), P("vocab", None), P("dp", "vocab")),
        out_specs=(P(("dp", "vocab")), P("vocab", None)),
        check_vma=False,
    )
```
